32 devices in a mesh: wide: 16 (over z, x, core), narrow: 2 (over y).
Axes of the slice: x: 2, y: 2, z: 4, core: 2. Of those that a mesh axis runs over, the one named last changes fastest.
Arguments:
- coords: float32 [3, 16, 2048], P(None, 'narrow', 'wide'), may hold values from -1 to 1
- member: int32 [16, 2048], P('narrow', 'wide'), may hold values 0 or 1
- start_vector: float32 [3, 16, 2048], P(None, 'narrow', 'wide'), may hold values from -6 to 6
- self_block: float32 [3, 3, 16, 2048], P(None, None, 'narrow', 'wide'), may hold values from -3 to 141
- neighbour_block: float32 [6, 3, 3, 16, 2048], P(None, None, None, 'narrow', 'wide'), may hold values from -3 to 3
- neighbours: int32 [6, 16, 2048], P(None, 'narrow', 'wide'), may hold values from 0 to 7, as said below
- coarse_map: int32 [512], replicated, may hold values from 0 to 511, each once
Outputs:
- smoothed: float32 [7, 6, 3, 16, 2048], P(None, None, None, 'narrow', 'wide')
- probe_vector: float32 [3, 16, 2048], P(None, 'narrow', 'wide')
- coarse_basis: float32 [36, 512], P(None, ('wide', 'narrow'))
The draws below stay inside these ranges and needn't reach their ends.
Inputs may be any that keep to these rules, and one draw needn't show every extreme that they name: `neighbours`: the 6 codes of each node are different. `coarse_map`: each aggregate number appears once.
All inputs are finite; a program needn't handle non-finite values. No bound on the sum of `member` on one device may be relied on, other than what follows from the above.
Results may differ from the reference program's by a relative error of at most 0.0003.
Values sent between devices are 32-bit elements; how exact they have to be, the bound alone decides.
A program may use at most 64 MiB of HBM per device.

```python
import math
import jax
import jax.numpy as jnp
from jax import lax

TILE = 8
NEIGH = 6
ITERS = 4
NODES_Y = 16
NODES_X = 2048
AGGREGATES = 512


def neighbour_draw(key):
    shape = (8, NODES_Y, NODES_X)
    scores = jax.random.randint(jax.random.fold_in(key, 11), shape, 0, 2 ** 20)
    ranked = scores * 8 + lax.broadcasted_iota(jnp.int32, shape, 0)
    ranking = jnp.argsort(ranked, axis=0, stable=True)
    return ranking[:NEIGH].astype(jnp.int32)


def operator_draw(key):
    chosen = neighbour_draw(key)
    spread = max(NODES_X - 1, 1)
    col_pos = lax.broadcasted_iota(jnp.float32, (NODES_Y, NODES_X), 1)
    stiffness = 1.0 + 2.0 * col_pos / spread
    shifted = chosen + (chosen >= 4).astype(jnp.int32)
    step_x = shifted % 3 - 1
    other_col = jnp.clip(lax.broadcasted_iota(jnp.int32, chosen.shape, 2) + step_x, 0, NODES_X - 1)
    other_stiff = 1.0 + 2.0 * other_col.astype(jnp.float32) / spread
    coupling = jnp.sqrt(stiffness[None] * other_stiff)
    neighbour_part = jax.random.uniform(jax.random.fold_in(key, 12), (NEIGH, 3, 3, NODES_Y, NODES_X), jnp.float32, -1.0, 1.0)
    neighbour_part = neighbour_part * coupling[:, None, None]
    self_off = jax.random.uniform(jax.random.fold_in(key, 13), (3, 3, NODES_Y, NODES_X), jnp.float32, -1.0, 1.0)
    extra = jnp.exp(jax.random.uniform(jax.random.fold_in(key, 14), (3, NODES_Y, NODES_X), jnp.float32, 0.0, math.log(24.0)))
    identity = jnp.eye(3, dtype=jnp.float32)[:, :, None, None]
    self_part = self_off * (1.0 - identity) + identity * (23.0 + extra)[:, None]
    self_part = self_part * stiffness[None, None]
    return (self_part, neighbour_part)


def draw_self_block(key, part):
    return operator_draw(key)[0]


def draw_neighbour_block(key, part):
    return operator_draw(key)[1]


def draw_neighbours(key, part):
    return neighbour_draw(key)


def plant(values, key, low, largest):
    place = [jax.random.randint(jax.random.fold_in(key, axis), (), 0, length) for axis, length in enumerate(values.shape)]
    main_axis = values.shape.index(max(values.shape))
    beside = place[:main_axis] + [(place[main_axis] + 1) % values.shape[main_axis]] + place[main_axis + 1:]
    return values.at[tuple(place)].set(low).at[tuple(beside)].set(largest)


def block_scale(rng, dims, split, smallest, largest):
    factor_of = 1.0
    for dim, shards_of in split:
        heights = jax.random.uniform(jax.random.fold_in(jax.random.fold_in(rng, 6), dim), (shards_of,), jnp.float32, smallest / len(split), largest / len(split))
        factor_of = factor_of * jnp.repeat(jnp.exp(heights), dims[dim] // shards_of).reshape((-1,) + (1,) * (len(dims) - 1 - dim))
    return factor_of


def bell_draw(key, shape, scale, most, cuts=(), kind=jnp.bfloat16):
    loudness = block_scale(key, shape, cuts, -0.22, 0.18) if cuts else 1.0
    values = jax.random.normal(key, shape, jnp.float32) * scale * loudness
    return jnp.minimum(jnp.maximum(values, -most), most).astype(kind)


def setup_inputs(seed: int = 0) -> dict:
    keys = jax.random.split(jax.random.key(seed), 8)
    coords = jnp.clip(jax.random.uniform(keys[0], (3, NODES_Y, NODES_X), jnp.float32, -1.0, 1.0) * block_scale(keys[0], (3, NODES_Y, NODES_X), ((1, 2), (2, 16)), -0.4, 0.0), -1.0, 1.0)
    member = plant((jax.random.randint(keys[1], (NODES_Y, NODES_X), 0, 4) < 3).astype(jnp.int32), jax.random.fold_in(keys[1], 1), 0, 1)
    start_vector = bell_draw(keys[2], (3, NODES_Y, NODES_X), 1.0, 6.0, ((1, 2), (2, 16)), jnp.float32)
    self_block = draw_self_block(jax.random.fold_in(keys[7], 71), 0)
    neighbour_block = draw_neighbour_block(jax.random.fold_in(keys[7], 71), 0)
    neighbours = draw_neighbours(jax.random.fold_in(keys[7], 71), 0)
    coarse_map = jax.random.permutation(keys[6], AGGREGATES).astype(jnp.int32)
    return {"coords": coords, "member": member, "start_vector": start_vector, "self_block": self_block, "neighbour_block": neighbour_block, "neighbours": neighbours, "coarse_map": coarse_map}


def edge_index(neighbours):
    edge_count, row_count, col_count = neighbours.shape
    shifted = neighbours + (neighbours >= 4).astype(jnp.int32)
    step_y = shifted // 3 - 1
    step_x = shifted % 3 - 1
    row_pos = lax.broadcasted_iota(jnp.int32, neighbours.shape, 1)
    col_pos = lax.broadcasted_iota(jnp.int32, neighbours.shape, 2)
    linear = (row_pos + 1 + step_y) * (col_count + 2) + (col_pos + 1 + step_x)
    return linear.reshape(edge_count, row_count * col_count).astype(jnp.int32)

def edge_pieces(extended, self_block, neighbour_block, lookup):
    mode_count, comp_count = (extended.shape[0], extended.shape[1])
    row_count, col_count = (self_block.shape[2], self_block.shape[3])
    centre = extended[:, :, 1:-1, 1:-1]
    flattened = extended.reshape(mode_count, comp_count, -1)
    pieces = [jnp.sum(self_block[None] * centre[:, None], axis=2)]
    for edge_id in range(lookup.shape[0]):
        picked = jnp.take(flattened, lookup[edge_id], axis=2).reshape(mode_count, comp_count, row_count, col_count)
        pieces.append(jnp.sum(neighbour_block[edge_id][None] * picked[:, None], axis=2))
    return pieces

def summed(pieces):
    result = pieces[0]
    for addend in pieces[1:]:
        result = result + addend
    return result

def build_tentative(coords, member):
    present = member.astype(jnp.float32)
    coord_x = coords[0] * present
    coord_y = coords[1] * present
    coord_z = coords[2] * present
    blanks = jnp.zeros_like(present)
    mode_basis = jnp.stack([jnp.stack([present, blanks, blanks]), jnp.stack([blanks, present, blanks]), jnp.stack([blanks, blanks, present]), jnp.stack([-coord_y, coord_x, blanks]), jnp.stack([blanks, -coord_z, coord_y]), jnp.stack([coord_z, blanks, -coord_x])])
    row_count, col_count = present.shape
    tiles_y, tiles_x = (row_count // TILE, col_count // TILE)
    tiled = mode_basis.reshape(6, 3, tiles_y, TILE, tiles_x, TILE)
    blocks = jnp.transpose(tiled, (2, 4, 0, 1, 3, 5)).reshape(tiles_y, tiles_x, 6, 3 * TILE * TILE)
    gram_matrix = jnp.einsum('yxmr,yxnr->yxmn', blocks, blocks, precision=lax.Precision.HIGHEST)
    factor_low = jnp.linalg.cholesky(gram_matrix)
    orthonormal = jax.scipy.linalg.solve_triangular(factor_low, blocks, lower=True)
    reshaped = orthonormal.reshape(tiles_y, tiles_x, 6, 3, TILE, TILE)
    tentative = jnp.transpose(reshaped, (2, 3, 0, 4, 1, 5)).reshape(6, 3, row_count, col_count)
    return (tentative, factor_low)

def padded(values):
    return jnp.pad(values, ((0, 0), (0, 0), (1, 1), (1, 1)))

def reference(coords, member, start_vector, self_block, neighbour_block, neighbours, coarse_map):
    lookup = edge_index(neighbours)
    diagonal = jnp.stack([self_block[0, 0], self_block[1, 1], self_block[2, 2]])
    tentative, factor_low = build_tentative(coords, member)
    iterate = start_vector[None]
    curvature = jnp.float32(1.0)
    energy = jnp.float32(1.0)
    for number in range(ITERS):
        applied = summed(edge_pieces(padded(iterate), self_block, neighbour_block, lookup))
        curvature = jnp.sum(iterate * applied)
        energy = jnp.sum(iterate * diagonal * iterate)
        iterate = energy / curvature * applied / diagonal
    jacobi_weight = 4.0 * energy / (3.0 * curvature)
    pieces = edge_pieces(padded(tentative), self_block, neighbour_block, lookup)
    weighting = jacobi_weight / diagonal
    smoothed = jnp.stack([tentative - weighting * pieces[0]] + [-weighting * portion for portion in pieces[1:]])
    factor_up = jnp.swapaxes(factor_low, 2, 3).reshape(-1, 36)
    coarse_basis = jnp.take(factor_up.T, coarse_map, axis=1)
    return (smoothed, iterate[0], coarse_basis)
```

```python
import functools

import jax
import jax.numpy as jnp
from jax import lax
from jax.experimental import pallas as pl
from jax.experimental.pallas import tpu as pltpu
from jax.sharding import PartitionSpec as P

TILE = 8
ITERS = 4
MESH = pl.DeviceIdType.MESH
F32 = jnp.float32
SUMS = 10
FIELDS = 9
STEPS = [(-1, -1), (-1, 0), (-1, 1), (0, -1), (0, 1), (1, -1), (1, 0), (1, 1)]


def roll(x, shift, axis):
    size = x.shape[axis]
    shift = shift % size
    return x if shift == 0 else pltpu.roll(x, shift, axis)


def displaced(v, lcol, rcol, rows, lane, row):
    height, width = v.shape
    first, last = lane == 0, lane == width - 1
    top, bottom = row == 0, row == height - 1
    vl = jnp.where(first, lcol, roll(v, 1, 1))
    vr = jnp.where(last, rcol, roll(v, -1, 1))
    w = jnp.where(bottom, rows[1], rows[6])
    wl = jnp.where(bottom, rows[0], rows[5])
    wr = jnp.where(bottom, rows[2], rows[7])
    wsl = roll(jnp.where(last, wl, w), 1, 1)
    wsr = roll(jnp.where(first, wr, w), -1, 1)
    up = [roll(jnp.where(bottom, b, a), 1, 0) for a, b in ((vl, wsl), (v, w), (vr, wsr))]
    down = [roll(jnp.where(top, b, a), -1, 0) for a, b in ((vl, wsl), (v, w), (vr, wsr))]
    return up + [vl, vr] + down


def kernel(
    wide, narrow, share,
    coords_h, member_h, start_h, self_h, nb_h, nbr_h, cmap_h,
    out_ref, probe_ref, coarse_ref,
    coords, member, selfb, nb, nbr, cmap,
    its, edges, stencil, fields, pack, tedges, disp, mine, gath, sumrow, allsum, partial,
    hrecv, vrecv, htrecv, vtrecv,
    in_sem, send_sem, recv_sem, tsend_sem, trecv_sem, gsend_sem, grecv_sem, ssend_sem, srecv_sem,
):
    count = wide * narrow
    me_w, me_n = lax.axis_index("wide"), lax.axis_index("narrow")
    me = me_w * narrow + me_n
    barrier = pltpu.get_barrier_semaphore()

    def peer(d):
        other = lax.rem(me + d, count)
        return (other // narrow, lax.rem(other, narrow))

    @pl.loop(1, count)
    def _(d):
        pl.semaphore_signal(barrier, inc=1, device_id=peer(d), device_id_type=MESH)

    loads = [
        pltpu.make_async_copy(src, dst, in_sem.at[i])
        for i, (src, dst) in enumerate(
            (
                (coords_h, coords), (member_h, member), (start_h, its.at[0]), (nbr_h, nbr),
                (self_h, selfb), (nb_h, nb), (cmap_h, cmap),
            )
        )
    ]
    for load in loads:
        load.start()

    def exists(code):
        dy, dx = STEPS[code]
        ok = None
        for step, at, size in ((dy, me_n, narrow), (dx, me_w, wide)):
            term = at > 0 if step < 0 else (at < size - 1 if step > 0 else None)
            if term is not None:
                ok = term if ok is None else jnp.logical_and(ok, term)
        return ok

    present_at = [exists(code) for code in range(8)]

    def target(code):
        dy, dx = STEPS[code]
        return (me_w + dx, me_n + dy)

    for code in range(8):
        @pl.when(jnp.logical_not(present_at[code]))
        def _(code=code):
            if code in (3, 4):
                hrecv[:, code - 3] = jnp.zeros(hrecv.shape[:1] + hrecv.shape[2:], F32)
                htrecv[code - 3] = jnp.zeros(htrecv.shape[1:], F32)
            else:
                vrecv[:, code] = jnp.zeros(vrecv.shape[:1] + vrecv.shape[2:], F32)
                vtrecv[code] = jnp.zeros(vtrecv.shape[1:], F32)

    shape = member.shape
    height, width = shape
    lane = lax.broadcasted_iota(jnp.int32, shape, 1)
    row = lax.broadcasted_iota(jnp.int32, shape, 0)

    def edge_rows(values, number):
        for r in range(3):
            edges[number, r : r + 1, :] = values[r][:1]
            edges[number, r + 4 : r + 5, :] = values[r][height - 1 :]

    for load in loads[:4]:
        load.wait()
    start = [its[0, r] for r in range(3)]
    edge_rows(start, 0)
    present = member[...].astype(F32)
    x, y, z = (coords[r] * present for r in range(3))
    products = [present * present, x * present, y * present, z * present, x * x, y * y, z * z, x * y, x * z, y * z]
    tiles = []
    for base in (0, 8):
        tile = jnp.zeros(shape, F32)
        for q, product in enumerate(products[base : base + 8]):
            tile = jnp.where(row == q, jnp.sum(product, axis=0, keepdims=True), tile)
        for s in (1, 2, 4):
            tile = tile + jnp.where((lane & s) != 0, roll(tile, s, 1), roll(tile, -s, 1))
        tiles.append(tile)
    sums = [tiles[q // 8][q % 8 : q % 8 + 1, :] for q in range(SUMS)]

    def factor(sums):
        n, sx, sy, sz, xx, yy, zz, xy, xz, yz = sums
        l00 = jnp.sqrt(n)
        mx, my, mz = sx / l00, sy / l00, sz / l00
        l33 = jnp.sqrt(xx + yy - mx * mx - my * my)
        l43 = (mx * mz - xz) / l33
        l53 = (my * mz - yz) / l33
        l44 = jnp.sqrt(yy + zz - my * my - mz * mz - l43 * l43)
        l54 = (mx * my - xy - l53 * l43) / l44
        l55 = jnp.sqrt(xx + zz - mx * mx - mz * mz - l53 * l53 - l54 * l54)
        return l00, mx, my, mz, l33, l43, l53, l44, l54, l55

    parts = factor(sums)
    l00, mx, my, mz, l33, l43, l53, l44, l54, l55 = parts
    unit = present / l00
    cx, cy, cz = x - mx * unit, y - my * unit, z - mz * unit
    a0, a1 = -cy / l33, cx / l33
    b0, b1, b2 = -l43 * a0 / l44, (-cz - l43 * a1) / l44, cy / l44
    g0 = (cz - l53 * a0 - l54 * b0) / l55
    g1 = (-l53 * a1 - l54 * b1) / l55
    g2 = (-cx - l54 * b2) / l55
    tent = [unit, a0, a1, b0, b1, b2, g0, g1, g2]
    packl, packr = jnp.zeros(shape, F32), jnp.zeros(shape, F32)
    for j, field in enumerate(tent):
        fields[j] = field
        packl = jnp.where(lane == j, roll(field, j, 1), packl)
        packr = jnp.where(lane == j, roll(field, j + 1, 1), packr)
        tedges[0, j : j + 1, :] = field[:1]
        tedges[1, j : j + 1, :] = field[height - 1 :]
    pack[0] = packl
    pack[1] = packr
    lane_row = lax.broadcasted_iota(jnp.int32, (1, width), 1) % 8
    rows_out = []
    for base in (0, 8):
        line = jnp.zeros((1, width), F32)
        for q, part in enumerate(parts[base : base + 8]):
            line = jnp.where(lane_row == q, part, line)
        rows_out.append(line)
    mine[0:1] = rows_out[0]
    mine[1:2] = rows_out[1]
    gath[me] = jnp.concatenate(rows_out, axis=0)

    pl.semaphore_wait(barrier, count - 1)

    def send_halo(number):
        copies = []
        for code in range(8):
            if code in (3, 4):
                src, dst = its.at[number], hrecv.at[number, 4 - code]
            else:
                src, dst = edges.at[number], vrecv.at[number, 7 - code]
            copy = pltpu.make_async_remote_copy(
                src_ref=src, dst_ref=dst, send_sem=send_sem.at[number, code], recv_sem=recv_sem.at[number, 7 - code],
                device_id=target(code), device_id_type=MESH,
            )
            pl.when(present_at[code])(copy.start)
            copies.append(copy)
        return copies

    def wait_halo(number, recv, hbuf, vbuf):
        for code in range(8):
            if code in (3, 4):
                ref = hbuf.at[code - 3]
            else:
                ref = vbuf.at[code]
            arrival = pltpu.make_async_copy(ref, ref, recv(code))
            pl.when(present_at[code])(arrival.wait)

    sent = [send_halo(0)]
    tcopies = []
    for code in range(8):
        if code in (3, 4):
            src, dst = pack.at[code - 3], htrecv.at[4 - code]
        else:
            src, dst = tedges.at[0 if code < 3 else 1], vtrecv.at[7 - code]
        copy = pltpu.make_async_remote_copy(
            src_ref=src, dst_ref=dst, send_sem=tsend_sem.at[code], recv_sem=trecv_sem.at[7 - code],
            device_id=target(code), device_id_type=MESH,
        )
        pl.when(present_at[code])(copy.start)
        tcopies.append(copy)

    @pl.loop(1, count)
    def _(d):
        pltpu.make_async_remote_copy(
            src_ref=mine, dst_ref=gath.at[me], send_sem=gsend_sem, recv_sem=grecv_sem,
            device_id=peer(d), device_id_type=MESH,
        ).start()

    for load in loads[4:]:
        load.wait()
    edge_count = nb.shape[0]
    for code in range(8):
        masks = [nbr[k] == code for k in range(edge_count)]
        for r in range(3):
            for s in range(3):
                value = jnp.zeros(shape, F32)
                for k in range(edge_count):
                    value = jnp.where(masks[k], nb[k, r, s], value)
                stencil[code, 3 * r + s] = value
    diag = [selfb[r, r] for r in range(3)]
    inv = [1.0 / d for d in diag]

    iterate = start
    for number in range(ITERS):
        wait_halo(number, lambda code: recv_sem.at[number, code], hrecv.at[number], vrecv.at[number])
        applied = [sum(selfb[r, s] * iterate[s] for s in range(3)) for r in range(3)]
        for s in range(3):
            rows = {
                code: vrecv[number, code, (s + 4 if code < 3 else s) : (s + 5 if code < 3 else s + 1), :]
                for code in (0, 1, 2, 5, 6, 7)
            }
            moved = displaced(
                iterate[s], roll(hrecv[number, 0, s], 1, 1), roll(hrecv[number, 1, s], -1, 1), rows, lane, row
            )
            for r in range(3):
                for code in range(8):
                    applied[r] = applied[r] + stencil[code, 3 * r + s] * moved[code]
        following = [applied[r] * inv[r] for r in range(3)]
        if number < ITERS - 1:
            for r in range(3):
                its[number + 1, r] = following[r]
            edge_rows(following, number + 1)
            sent.append(send_halo(number + 1))
        curvature = sum(iterate[r] * applied[r] for r in range(3))
        energy = sum(iterate[r] * diag[r] * iterate[r] for r in range(3))
        partial[number : number + 1] = jnp.sum(curvature, axis=0, keepdims=True)
        partial[number + 4 : number + 5] = jnp.sum(energy, axis=0, keepdims=True)
        iterate = following

    totals = jnp.sum(partial[...], axis=1, keepdims=True)
    line = jnp.sum(jnp.where(lane == row, totals, 0.0), axis=0, keepdims=True)
    sumrow[...] = line
    allsum[me] = line

    @pl.loop(1, count)
    def _(d):
        pltpu.make_async_remote_copy(
            src_ref=sumrow, dst_ref=allsum.at[me], send_sem=ssend_sem, recv_sem=srecv_sem,
            device_id=peer(d), device_id_type=MESH,
        ).start()

    wait_halo(0, lambda code: trecv_sem.at[code], htrecv, vtrecv)
    lpack, rpack = htrecv[0], htrecv[1]
    for j in range(FIELDS):
        rows = {code: vtrecv[code, j : j + 1, :] for code in (0, 1, 2, 5, 6, 7)}
        moved = displaced(tent[j], roll(lpack, -j, 1), roll(rpack, width - 1 - j, 1), rows, lane, row)
        for code in range(8):
            disp[j, code] = moved[code]

    def piece(block, picked, index):
        unit, a0, a1, b0, b1, b2, g0, g1, g2 = picked
        for r in range(3):
            c0, c1, c2 = (block(r, s) * -inv[r] for s in range(3))
            out_ref[index, 0, r] = c0 * unit
            out_ref[index, 1, r] = c1 * unit
            out_ref[index, 2, r] = c2 * unit
            out_ref[index, 3, r] = c0 * a0 + c1 * a1
            out_ref[index, 4, r] = c0 * b0 + c1 * b1 + c2 * b2
            out_ref[index, 5, r] = c0 * g0 + c1 * g1 + c2 * g2

    piece(lambda r, s: selfb[r, s], [fields[j] for j in range(FIELDS)], 0)
    for k in range(edge_count):
        masks = [nbr[k] == code for code in range(1, 8)]
        picked = []
        for j in range(FIELDS):
            value = disp[j, 0]
            for code in range(1, 8):
                value = jnp.where(masks[code - 1], disp[j, code], value)
            picked.append(value)
        piece(lambda r, s: nb[k, r, s], picked, k + 1)

    some = gath.at[pl.ds(0, count - 1)]
    pltpu.make_async_copy(some, some, grecv_sem).wait()
    across = width // TILE * wide
    tiles_x, tiles_y = width // TILE, height // TILE
    crow = lax.broadcasted_iota(jnp.int32, (share, width), 0)
    cgroup = lax.broadcasted_iota(jnp.int32, (share, width), 1) // TILE
    low, high = jnp.zeros((share, width), F32), jnp.zeros((share, width), F32)
    for j in range(share):
        wanted = cmap[me * share + j]
        tile_row, tile_col = wanted // across, lax.rem(wanted, across)
        slot = tile_col // tiles_x * narrow + tile_row // tiles_y
        lines = gath[slot]
        take = jnp.logical_and(crow == j, cgroup == lax.rem(tile_col, tiles_x))
        low = jnp.where(take, lines[0:1], low)
        high = jnp.where(take, lines[1:2], high)
    pick = (lax.broadcasted_iota(jnp.int32, (8, width), 1) % 8 == lax.broadcasted_iota(jnp.int32, (8, width), 0)).astype(F32)
    low, high = (
        lax.dot_general(
            pick, v, (((1,), (1,)), ((), ())), precision=lax.Precision.HIGHEST, preferred_element_type=F32
        )
        for v in (low, high)
    )
    l00, mx, my, mz, l33, l43, l53, l44 = (low[q : q + 1] for q in range(8))
    l54, l55 = high[0:1], high[1:2]
    coarse_ref[...] = jnp.zeros(coarse_ref.shape, F32)
    entries = {
        (0, 0): l00, (1, 1): l00, (2, 2): l00,
        (3, 0): -my, (3, 1): mx, (4, 1): -mz, (4, 2): my, (5, 0): mz, (5, 2): -mx,
        (3, 3): l33, (4, 3): l43, (5, 3): l53, (4, 4): l44, (5, 4): l54, (5, 5): l55,
    }
    for (n, m), entry in entries.items():
        coarse_ref[6 * m + n : 6 * m + n + 1, :] = entry

    some = allsum.at[pl.ds(0, count - 1)]
    pltpu.make_async_copy(some, some, srecv_sem).wait()
    if count <= 64:
        lines = [allsum[d] for d in range(count)]
        while len(lines) > 1:
            lines = [a + b for a, b in zip(lines[::2], lines[1::2])] + ([lines[-1]] if len(lines) % 2 else [])
        total = lines[0]
    else:
        total = lax.fori_loop(0, count, lambda d, t: t + allsum[d], jnp.zeros((1, width), F32))
    lane1 = lax.broadcasted_iota(jnp.int32, (1, width), 1)
    ratio = roll(jnp.broadcast_to(total, shape), -4, 1)[:1] / total
    ratios = [jnp.sum(jnp.where(lane1 == i, ratio, 0.0), axis=1, keepdims=True) for i in range(ITERS)]
    growth = ratios[0]
    for i in range(1, ITERS):
        growth = growth * ratios[i]
    weight = jnp.broadcast_to(ratios[ITERS - 1] * (4.0 / 3.0), shape)
    growth = jnp.broadcast_to(growth, shape)
    for r in range(3):
        probe_ref[r] = iterate[r] * growth
    base = {(0, 0): 0, (1, 1): 0, (2, 2): 0, (3, 0): 1, (3, 1): 2}
    for r in range(3):
        base[(4, r)] = 3 + r
        base[(5, r)] = 6 + r
    for m in range(6):
        for r in range(3):
            value = out_ref[0, m, r] * weight
            out_ref[0, m, r] = value + fields[base[(m, r)]] if (m, r) in base else value
    for k in range(1, edge_count + 1):
        for m in range(6):
            for r in range(3):
                out_ref[k, m, r] = out_ref[k, m, r] * weight

    for copies in sent + [tcopies]:
        for code in range(8):
            pl.when(present_at[code])(copies[code].wait_send)
    for buffer, sem in ((gath, gsend_sem), (allsum, ssend_sem)):
        some = buffer.at[pl.ds(0, count - 1)]
        pltpu.make_async_copy(some, some, sem).wait()


def local(wide, narrow, coords, member, start_vector, self_block, neighbour_block, neighbours, coarse_map):
    height, width = member.shape
    edge_count = neighbours.shape[0]
    count = wide * narrow
    share = coarse_map.shape[0] // count
    tile = (height, width)
    vmem = pltpu.VMEM
    dma = pltpu.SemaphoreType.DMA
    return pl.pallas_call(
        functools.partial(kernel, wide, narrow, share),
        out_shape=(
            jax.ShapeDtypeStruct((edge_count + 1, 6, 3) + tile, F32),
            jax.ShapeDtypeStruct((3,) + tile, F32),
            jax.ShapeDtypeStruct((36, share), F32),
        ),
        in_specs=[pl.BlockSpec(memory_space=pl.ANY)] * 7,
        out_specs=(pl.BlockSpec(memory_space=pltpu.VMEM),) * 3,
        scratch_shapes=[
            vmem((3,) + tile, F32),
            vmem(tile, jnp.int32),
            vmem((3, 3) + tile, F32),
            vmem((edge_count, 3, 3) + tile, F32),
            vmem((edge_count,) + tile, jnp.int32),
            pltpu.SMEM(coarse_map.shape, jnp.int32),
            vmem((ITERS, 3) + tile, F32),
            vmem((ITERS, 8, width), F32),
            vmem((8, 9) + tile, F32),
            vmem((FIELDS,) + tile, F32),
            vmem((2,) + tile, F32),
            vmem((2, 16, width), F32),
            vmem((FIELDS, 8) + tile, F32),
            vmem((2, width), F32),
            vmem((count, 2, width), F32),
            vmem((1, width), F32),
            vmem((count, 1, width), F32),
            vmem((8, width), F32),
            vmem((ITERS, 2, 3) + tile, F32),
            vmem((ITERS, 8, 8, width), F32),
            vmem((2,) + tile, F32),
            vmem((8, 16, width), F32),
            dma((7,)),
            dma((ITERS, 8)),
            dma((ITERS, 8)),
            dma((8,)),
            dma((8,)),
            dma(()),
            dma(()),
            dma(()),
            dma(()),
        ],
        compiler_params=pltpu.CompilerParams(collective_id=0, has_side_effects=True),
    )(coords, member, start_vector, self_block, neighbour_block, neighbours, coarse_map)


def solution(mesh):
    return jax.shard_map(
        functools.partial(local, mesh.shape["wide"], mesh.shape["narrow"]),
        mesh=mesh,
        in_specs=(
            P(None, "narrow", "wide"),
            P("narrow", "wide"),
            P(None, "narrow", "wide"),
            P(None, None, "narrow", "wide"),
            P(None, None, None, "narrow", "wide"),
            P(None, "narrow", "wide"),
            P(),
        ),
        out_specs=(
            P(None, None, None, "narrow", "wide"),
            P(None, "narrow", "wide"),
            P(None, ("wide", "narrow")),
        ),
        check_vma=False,
    )
```

```python
import functools

import jax
import jax.numpy as jnp
from jax import lax
from jax.experimental import pallas as pl
from jax.experimental.pallas import tpu as pltpu
from jax.sharding import PartitionSpec as P

TILE = 8
ITERS = 4
MESH = pl.DeviceIdType.MESH
F32 = jnp.float32
SUMS = 10
FIELDS = 9
START, SELF, NB = 0, 3, 12
STEPS = [(-1, -1), (-1, 0), (-1, 1), (0, -1), (0, 1), (1, -1), (1, 0), (1, 1)]


def roll(x, shift, axis):
    size = x.shape[axis]
    shift = shift % size
    return x if shift == 0 else pltpu.roll(x, shift, axis)


def displaced(v, lcol, rcol, rows, lane, row):
    height, width = v.shape
    first, last = lane == 0, lane == width - 1
    top, bottom = row == 0, row == height - 1
    vl = jnp.where(first, lcol, roll(v, 1, 1))
    vr = jnp.where(last, rcol, roll(v, -1, 1))
    w = jnp.where(bottom, rows[1], rows[6])
    wl = jnp.where(bottom, rows[0], rows[5])
    wr = jnp.where(bottom, rows[2], rows[7])
    wsl = roll(jnp.where(last, wl, w), 1, 1)
    wsr = roll(jnp.where(first, wr, w), -1, 1)
    up = [roll(jnp.where(bottom, b, a), 1, 0) for a, b in ((vl, wsl), (v, w), (vr, wsr))]
    down = [roll(jnp.where(top, b, a), -1, 0) for a, b in ((vl, wsl), (v, w), (vr, wsr))]
    return up + [vl, vr] + down


def kernel(
    wide, narrow, share,
    coords_h, member_h, start_h, self_h, nb_h, nbr_h, cmap_h,
    out_ref, probe_ref, coarse_ref,
    coords, member, nbr, cmap,
    ext, wpack, stencil, fields, pack, tedges, disp, mine, gath, sumrow, allsum, partial,
    wrecv, htrecv, vtrecv,
    in_sem, send_sem, recv_sem, tsend_sem, trecv_sem, gsend_sem, grecv_sem, ssend_sem, srecv_sem,
):
    count = wide * narrow
    me_w, me_n = lax.axis_index("wide"), lax.axis_index("narrow")
    me = me_w * narrow + me_n
    barrier = pltpu.get_barrier_semaphore()

    def peer(d):
        other = lax.rem(me + d, count)
        return (other // narrow, lax.rem(other, narrow))

    @pl.loop(1, count)
    def _(d):
        pl.semaphore_signal(barrier, inc=1, device_id=peer(d), device_id_type=MESH)

    height, width = shape = member.shape
    edge_count = nbr.shape[0]
    codes_at = NB + 9 * edge_count
    planes = codes_at + edge_count

    def own(first, size):
        return ext.at[first : first + size, 0:height, 0:width]

    loads = [
        pltpu.make_async_copy(src, dst, in_sem.at[i])
        for i, (src, dst) in enumerate(
            (
                (nbr_h, nbr), (start_h, own(START, 3)), (self_h, own(SELF, 9)), (nb_h, own(NB, nb_h.shape[0])),
                (coords_h, coords), (member_h, member), (cmap_h, cmap),
            )
        )
    ]
    for load in loads:
        load.start()

    def exists(code):
        dy, dx = STEPS[code]
        ok = None
        for step, at, size in ((dy, me_n, narrow), (dx, me_w, wide)):
            term = at > 0 if step < 0 else (at < size - 1 if step > 0 else None)
            if term is not None:
                ok = term if ok is None else jnp.logical_and(ok, term)
        return ok

    present_at = [exists(code) for code in range(8)]

    def target(code):
        dy, dx = STEPS[code]
        return (me_w + dx, me_n + dy)

    for code in range(8):
        @pl.when(jnp.logical_not(present_at[code]))
        def _(code=code):
            if code in (1, 6):
                at = height + ITERS if code == 1 else height
                ext[:, at : at + ITERS, 0:width] = jnp.zeros((planes, ITERS, width), F32)
            else:
                wrecv[code] = jnp.zeros(wrecv.shape[1:], F32)
            if code in (3, 4):
                htrecv[code - 3] = jnp.zeros(htrecv.shape[1:], F32)
            else:
                vtrecv[code] = jnp.zeros(vtrecv.shape[1:], F32)

    lane = lax.broadcasted_iota(jnp.int32, shape, 1)
    row = lax.broadcasted_iota(jnp.int32, shape, 0)

    for load in loads[:4]:
        load.wait()
    for k in range(edge_count):
        ext[codes_at + k, 0:height, 0:width] = nbr[k].astype(F32)
    per = width // ITERS
    for side in range(2):
        for t in range(wpack.shape[1]):
            tile = jnp.zeros(shape, F32)
            for j, p in enumerate(range(t * per, min((t + 1) * per, planes))):
                moved = roll(ext[p, 0:height, 0:width], ITERS * (j + side), 1)
                tile = jnp.where(lane // ITERS == j, moved, tile)
            wpack[side, t] = tile

    pl.semaphore_wait(barrier, count - 1)

    copies = []
    for code in range(8):
        dx = STEPS[code][1]
        if dx == 0:
            here, there = (0, height) if code == 1 else (height - ITERS, height + ITERS)
            src = ext.at[:, here : here + ITERS, 0:width]
            dst = ext.at[:, there : there + ITERS, 0:width]
        else:
            src, dst = wpack.at[0 if dx < 0 else 1], wrecv.at[7 - code]
        copy = pltpu.make_async_remote_copy(
            src_ref=src, dst_ref=dst, send_sem=send_sem.at[code], recv_sem=recv_sem.at[7 - code],
            device_id=target(code), device_id_type=MESH,
        )
        pl.when(present_at[code])(copy.start)
        copies.append(copy)

    for load in loads[4:]:
        load.wait()
    present = member[...].astype(F32)
    x, y, z = (coords[r] * present for r in range(3))
    products = [present * present, x * present, y * present, z * present, x * x, y * y, z * z, x * y, x * z, y * z]
    tiles = []
    for base in (0, 8):
        tile = jnp.zeros(shape, F32)
        for q, product in enumerate(products[base : base + 8]):
            tile = jnp.where(row == q, jnp.sum(product, axis=0, keepdims=True), tile)
        for s in (1, 2, 4):
            tile = tile + jnp.where((lane & s) != 0, roll(tile, s, 1), roll(tile, -s, 1))
        tiles.append(tile)
    sums = [tiles[q // 8][q % 8 : q % 8 + 1, :] for q in range(SUMS)]

    def factor(sums):
        n, sx, sy, sz, xx, yy, zz, xy, xz, yz = sums
        l00 = jnp.sqrt(n)
        mx, my, mz = sx / l00, sy / l00, sz / l00
        l33 = jnp.sqrt(xx + yy - mx * mx - my * my)
        l43 = (mx * mz - xz) / l33
        l53 = (my * mz - yz) / l33
        l44 = jnp.sqrt(yy + zz - my * my - mz * mz - l43 * l43)
        l54 = (mx * my - xy - l53 * l43) / l44
        l55 = jnp.sqrt(xx + zz - mx * mx - mz * mz - l53 * l53 - l54 * l54)
        return l00, mx, my, mz, l33, l43, l53, l44, l54, l55

    parts = factor(sums)
    l00, mx, my, mz, l33, l43, l53, l44, l54, l55 = parts
    unit = present / l00
    cx, cy, cz = x - mx * unit, y - my * unit, z - mz * unit
    a0, a1 = -cy / l33, cx / l33
    b0, b1, b2 = -l43 * a0 / l44, (-cz - l43 * a1) / l44, cy / l44
    g0 = (cz - l53 * a0 - l54 * b0) / l55
    g1 = (-l53 * a1 - l54 * b1) / l55
    g2 = (-cx - l54 * b2) / l55
    tent = [unit, a0, a1, b0, b1, b2, g0, g1, g2]
    packl, packr = jnp.zeros(shape, F32), jnp.zeros(shape, F32)
    for j, field in enumerate(tent):
        fields[j] = field
        packl = jnp.where(lane == j, roll(field, j, 1), packl)
        packr = jnp.where(lane == j, roll(field, j + 1, 1), packr)
        tedges[0, j : j + 1, :] = field[:1]
        tedges[1, j : j + 1, :] = field[height - 1 :]
    pack[0] = packl
    pack[1] = packr
    lane_row = lax.broadcasted_iota(jnp.int32, (1, width), 1) % 8
    rows_out = []
    for base in (0, 8):
        line = jnp.zeros((1, width), F32)
        for q, part in enumerate(parts[base : base + 8]):
            line = jnp.where(lane_row == q, part, line)
        rows_out.append(line)
    mine[0:1] = rows_out[0]
    mine[1:2] = rows_out[1]
    gath[me] = jnp.concatenate(rows_out, axis=0)

    def wait_halo(codes, recv, ref_of):
        for code in codes:
            ref = ref_of(code)
            arrival = pltpu.make_async_copy(ref, ref, recv.at[code])
            pl.when(present_at[code])(arrival.wait)

    tcopies = []
    for code in range(8):
        if code in (3, 4):
            src, dst = pack.at[code - 3], htrecv.at[4 - code]
        else:
            src, dst = tedges.at[0 if code < 3 else 1], vtrecv.at[7 - code]
        copy = pltpu.make_async_remote_copy(
            src_ref=src, dst_ref=dst, send_sem=tsend_sem.at[code], recv_sem=trecv_sem.at[7 - code],
            device_id=target(code), device_id_type=MESH,
        )
        pl.when(present_at[code])(copy.start)
        tcopies.append(copy)

    @pl.loop(1, count)
    def _(d):
        pltpu.make_async_remote_copy(
            src_ref=mine, dst_ref=gath.at[me], send_sem=gsend_sem, recv_sem=grecv_sem,
            device_id=peer(d), device_id_type=MESH,
        ).start()

    def by_displacement(r0, c0):
        def at(p):
            return ext[p, r0 : r0 + height, c0 : c0 + width]

        for code in range(8):
            masks = [at(codes_at + k) == code for k in range(edge_count)]
            for q in range(9):
                value = jnp.zeros(shape, F32)
                for k in range(edge_count):
                    value = jnp.where(masks[k], at(NB + 9 * k + q), value)
                stencil[code, q, r0 : r0 + height, c0 : c0 + width] = value

    def ring(code):
        at = height + ITERS if code == 1 else height
        return ext.at[:, at : at + ITERS, 0:width]

    by_displacement(0, 0)
    wait_halo((1, 6), recv_sem, ring)
    by_displacement(height, 0)
    wait_halo((0, 2, 3, 4, 5, 7), recv_sem, lambda code: wrecv.at[code])
    half = row < ITERS
    for t in range(wpack.shape[1]):
        pairs = (
            (wrecv[4, t], wrecv[3, t]),
            (jnp.where(half, wrecv[7, t], wrecv[2, t]), jnp.where(half, wrecv[5, t], wrecv[0, t])),
        )
        for j, p in enumerate(range(t * per, min((t + 1) * per, planes))):
            for r0, (right, left) in zip((0, height), pairs):
                tile = jnp.where(lane >= width - ITERS, roll(left, -ITERS * (j + 1), 1), 0.0)
                ext[p, r0 : r0 + height, width:] = jnp.where(lane < ITERS, roll(right, -ITERS * j, 1), tile)
    by_displacement(0, width)
    by_displacement(height, width)

    def full(p):
        return ext[p]

    selfb = {(r, s): (lambda r=r, s=s: ext[SELF + 3 * r + s, 0:height, 0:width]) for r in range(3) for s in range(3)}
    nb = {
        (k, r, s): (lambda k=k, r=r, s=s: ext[NB + 9 * k + 3 * r + s, 0:height, 0:width])
        for k in range(edge_count) for r in range(3) for s in range(3)
    }
    elane = lax.broadcasted_iota(jnp.int32, (2 * height, 2 * width), 1)
    erow = lax.broadcasted_iota(jnp.int32, (2 * height, 2 * width), 0)

    def between(value, low, high):
        return jnp.logical_and(value >= low, value < high)

    last_row = jnp.where(me_n < narrow - 1, height + ITERS, height)
    back_row = jnp.where(me_n > 0, height + ITERS, 2 * height)
    last_lane = jnp.where(me_w < wide - 1, width + ITERS, width)
    back_lane = jnp.where(me_w > 0, 2 * width - ITERS, 2 * width)
    inside = jnp.logical_and(
        jnp.logical_or(erow < last_row, erow >= back_row), jnp.logical_or(elane < last_lane, elane >= back_lane)
    )
    inverse = [jnp.where(inside, 1.0 / full(SELF + 4 * r), 0.0) for r in range(3)]
    diag = [selfb[r, r]() for r in range(3)]
    inv = [inverse[r][:height, :width] for r in range(3)]

    iterate = [full(START + r) for r in range(3)]
    for number in range(ITERS):
        final = number == ITERS - 1
        rs, cs = (slice(0, height), slice(0, width)) if final else (slice(None), slice(None))
        applied = [sum(ext[SELF + 3 * r + s, rs, cs] * iterate[s][rs, cs] for s in range(3)) for r in range(3)]
        for s in range(3):
            for dy in (-1, 0, 1):
                shifted = roll(iterate[s], -dy, 0)
                for dx in (-1, 0, 1):
                    if (dy, dx) == (0, 0):
                        continue
                    code = STEPS.index((dy, dx))
                    moved = roll(shifted, -dx, 1)[rs, cs]
                    for r in range(3):
                        applied[r] = applied[r] + stencil[code, 3 * r + s, rs, cs] * moved
        mine_it = [v[:height, :width] for v in iterate]
        mine_ap = [v[:height, :width] for v in applied]
        curvature = sum(mine_it[r] * mine_ap[r] for r in range(3))
        energy = sum(mine_it[r] * diag[r] * mine_it[r] for r in range(3))
        partial[number : number + 1] = jnp.sum(curvature, axis=0, keepdims=True)
        partial[number + 4 : number + 5] = jnp.sum(energy, axis=0, keepdims=True)
        iterate = [applied[r] * (inv[r] if final else inverse[r]) for r in range(3)]

    totals = jnp.sum(partial[...], axis=1, keepdims=True)
    line = jnp.sum(jnp.where(lane == row, totals, 0.0), axis=0, keepdims=True)
    sumrow[...] = line
    allsum[me] = line

    @pl.loop(1, count)
    def _(d):
        pltpu.make_async_remote_copy(
            src_ref=sumrow, dst_ref=allsum.at[me], send_sem=ssend_sem, recv_sem=srecv_sem,
            device_id=peer(d), device_id_type=MESH,
        ).start()

    wait_halo(range(8), trecv_sem, lambda code: htrecv.at[code - 3] if code in (3, 4) else vtrecv.at[code])
    lpack, rpack = htrecv[0], htrecv[1]
    for j in range(FIELDS):
        rows = {code: vtrecv[code, j : j + 1, :] for code in (0, 1, 2, 5, 6, 7)}
        moved = displaced(tent[j], roll(lpack, -j, 1), roll(rpack, width - 1 - j, 1), rows, lane, row)
        for code in range(8):
            disp[j, code] = moved[code]

    def piece(block, picked, index):
        unit, a0, a1, b0, b1, b2, g0, g1, g2 = picked
        for r in range(3):
            c0, c1, c2 = (block(r, s) * -inv[r] for s in range(3))
            out_ref[index, 0, r] = c0 * unit
            out_ref[index, 1, r] = c1 * unit
            out_ref[index, 2, r] = c2 * unit
            out_ref[index, 3, r] = c0 * a0 + c1 * a1
            out_ref[index, 4, r] = c0 * b0 + c1 * b1 + c2 * b2
            out_ref[index, 5, r] = c0 * g0 + c1 * g1 + c2 * g2

    piece(lambda r, s: selfb[r, s](), [fields[j] for j in range(FIELDS)], 0)
    for k in range(edge_count):
        masks = [nbr[k] == code for code in range(1, 8)]
        picked = []
        for j in range(FIELDS):
            value = disp[j, 0]
            for code in range(1, 8):
                value = jnp.where(masks[code - 1], disp[j, code], value)
            picked.append(value)
        piece(lambda r, s: nb[k, r, s](), picked, k + 1)

    some = gath.at[pl.ds(0, count - 1)]
    pltpu.make_async_copy(some, some, grecv_sem).wait()
    across = width // TILE * wide
    tiles_x, tiles_y = width // TILE, height // TILE
    crow = lax.broadcasted_iota(jnp.int32, (share, width), 0)
    cgroup = lax.broadcasted_iota(jnp.int32, (share, width), 1) // TILE
    low, high = jnp.zeros((share, width), F32), jnp.zeros((share, width), F32)
    for j in range(share):
        wanted = cmap[me * share + j]
        tile_row, tile_col = wanted // across, lax.rem(wanted, across)
        slot = tile_col // tiles_x * narrow + tile_row // tiles_y
        lines = gath[slot]
        take = jnp.logical_and(crow == j, cgroup == lax.rem(tile_col, tiles_x))
        low = jnp.where(take, lines[0:1], low)
        high = jnp.where(take, lines[1:2], high)
    l00, mx, my, mz, l33, l43, l53, l44, l54, l55 = range(SUMS)
    entries = {
        (0, 0): (l00, 1), (1, 1): (l00, 1), (2, 2): (l00, 1),
        (3, 0): (my, -1), (3, 1): (mx, 1), (4, 1): (mz, -1), (4, 2): (my, 1), (5, 0): (mz, 1), (5, 2): (mx, -1),
        (3, 3): (l33, 1), (4, 3): (l43, 1), (5, 3): (l53, 1), (4, 4): (l44, 1), (5, 4): (l54, 1), (5, 5): (l55, 1),
    }
    outs = coarse_ref.shape[1]
    kind = lax.broadcasted_iota(jnp.int32, (1, outs), 1)
    chosen, sign = jnp.full((1, outs), -1, jnp.int32), jnp.zeros((1, outs), F32)
    for (n, m), (q, way) in entries.items():
        chosen = jnp.where(kind == 6 * m + n, q, chosen)
        sign = jnp.where(kind == 6 * m + n, float(way), sign)
    entry = lax.broadcasted_iota(jnp.int32, (width, outs), 0) % 8
    coarse = jnp.zeros(coarse_ref.shape, F32)
    for base, lines in ((0, low), (8, high)):
        pick = jnp.where(entry + base == chosen, sign, 0.0)
        coarse = coarse + jnp.dot(lines, pick, precision=lax.Precision.HIGHEST, preferred_element_type=F32)
    coarse_ref[...] = coarse

    some = allsum.at[pl.ds(0, count - 1)]
    pltpu.make_async_copy(some, some, srecv_sem).wait()
    if count <= 64:
        lines = [allsum[d] for d in range(count)]
        while len(lines) > 1:
            lines = [a + b for a, b in zip(lines[::2], lines[1::2])] + ([lines[-1]] if len(lines) % 2 else [])
        total = lines[0]
    else:
        total = lax.fori_loop(0, count, lambda d, t: t + allsum[d], jnp.zeros((1, width), F32))
    lane1 = lax.broadcasted_iota(jnp.int32, (1, width), 1)
    ratio = roll(jnp.broadcast_to(total, shape), -4, 1)[:1] / total
    ratios = [jnp.sum(jnp.where(lane1 == i, ratio, 0.0), axis=1, keepdims=True) for i in range(ITERS)]
    growth = ratios[0]
    for i in range(1, ITERS):
        growth = growth * ratios[i]
    weight = jnp.broadcast_to(ratios[ITERS - 1] * (4.0 / 3.0), shape)
    growth = jnp.broadcast_to(growth, shape)
    for r in range(3):
        probe_ref[r] = iterate[r] * growth
    base = {(0, 0): 0, (1, 1): 0, (2, 2): 0, (3, 0): 1, (3, 1): 2}
    for r in range(3):
        base[(4, r)] = 3 + r
        base[(5, r)] = 6 + r
    for m in range(6):
        for r in range(3):
            value = out_ref[0, m, r] * weight
            out_ref[0, m, r] = value + fields[base[(m, r)]] if (m, r) in base else value
    for k in range(1, edge_count + 1):
        for m in range(6):
            for r in range(3):
                out_ref[k, m, r] = out_ref[k, m, r] * weight

    for some in (copies, tcopies):
        for code in range(8):
            pl.when(present_at[code])(some[code].wait_send)
    for buffer, sem in ((gath, gsend_sem), (allsum, ssend_sem)):
        some = buffer.at[pl.ds(0, count - 1)]
        pltpu.make_async_copy(some, some, sem).wait()


def local(wide, narrow, coords, member, start_vector, self_block, neighbour_block, neighbours, coarse_map):
    height, width = member.shape
    edge_count = neighbours.shape[0]
    count = wide * narrow
    share = coarse_map.shape[0] // count
    tile = (height, width)
    double = (2 * height, 2 * width)
    planes = 12 + 10 * edge_count
    packs = pl.cdiv(planes, width // ITERS)
    vmem = pltpu.VMEM
    dma = pltpu.SemaphoreType.DMA
    smoothed, probe, coarse = pl.pallas_call(
        functools.partial(kernel, wide, narrow, share),
        out_shape=(
            jax.ShapeDtypeStruct((edge_count + 1, 6, 3) + tile, F32),
            jax.ShapeDtypeStruct((3,) + tile, F32),
            jax.ShapeDtypeStruct((share, 36), F32),
        ),
        in_specs=[pl.BlockSpec(memory_space=pl.ANY)] * 7,
        out_specs=(pl.BlockSpec(memory_space=pltpu.VMEM),) * 3,
        scratch_shapes=[
            vmem((3,) + tile, F32),
            vmem(tile, jnp.int32),
            vmem((edge_count,) + tile, jnp.int32),
            pltpu.SMEM(coarse_map.shape, jnp.int32),
            vmem((planes,) + double, F32),
            vmem((2, packs) + tile, F32),
            vmem((8, 9) + double, F32),
            vmem((FIELDS,) + tile, F32),
            vmem((2,) + tile, F32),
            vmem((2, 16, width), F32),
            vmem((FIELDS, 8) + tile, F32),
            vmem((2, width), F32),
            vmem((count, 2, width), F32),
            vmem((1, width), F32),
            vmem((count, 1, width), F32),
            vmem((8, width), F32),
            vmem((8, packs) + tile, F32),
            vmem((2,) + tile, F32),
            vmem((8, 16, width), F32),
            dma((7,)),
            dma((8,)),
            dma((8,)),
            dma((8,)),
            dma((8,)),
            dma(()),
            dma(()),
            dma(()),
            dma(()),
        ],
        compiler_params=pltpu.CompilerParams(collective_id=0, has_side_effects=True),
    )(
        coords, member, start_vector, self_block.reshape((9,) + tile), neighbour_block.reshape((-1,) + tile),
        neighbours, coarse_map,
    )
    return smoothed, probe, coarse.T


def solution(mesh):
    return jax.shard_map(
        functools.partial(local, mesh.shape["wide"], mesh.shape["narrow"]),
        mesh=mesh,
        in_specs=(
            P(None, "narrow", "wide"),
            P("narrow", "wide"),
            P(None, "narrow", "wide"),
            P(None, None, "narrow", "wide"),
            P(None, None, None, "narrow", "wide"),
            P(None, "narrow", "wide"),
            P(),
        ),
        out_specs=(
            P(None, None, None, "narrow", "wide"),
            P(None, "narrow", "wide"),
            P(None, ("wide", "narrow")),
        ),
        check_vma=False,
    )
```
